128 devices in a mesh: grp: 4 (over z_lo, core), tile: 32 (over x, z_hi, y).
Axes of the slice: x: 4, y: 4, z: 4 (z_hi: 2, z_lo: 2; z = z_hi * 2 + z_lo), core: 2. Of those that a mesh axis runs over, the one named last changes fastest.
Arguments:
- amplitudes: bfloat16 [160, 4, 983040], P(None, None, ('grp', 'tile')), may hold values from -6 to 6
- w_vvvo: bfloat16 [1024, 983040], P(None, ('grp', 'tile')), may hold values from -0.0234375 to 0.0234375
- pair_mask: int32 [4096], P(('grp', 'tile')), may hold values from 0 to 1, as said below
- owner_map: int32 [32], replicated, may hold values from 0 to 31, each once
Outputs:
- sigma_one: float32 [160, 4, 1024], P('tile', None, 'grp')
The draws below stay inside these ranges and needn't reach their ends.
Inputs may be any that keep to these rules, and one draw needn't show every extreme that they name: `pair_mask`: in each aligned block of 32 pairs at most 24 are 1 and at least one is; some block has exactly 24 and some block exactly one. `owner_map`: a permutation of the row blocks.
All inputs are finite; a program needn't handle non-finite values.
Results may differ from the reference program's by a relative error of at most 0.0003.
Values sent between devices are 32-bit elements; how exact they have to be, the bound alone decides.
No kernel may reach another device: no remote copies, remote signals or barrier semaphores. Data moves between devices by JAX's collectives and lax.ppermute only.
A program may use at most 128 MiB of HBM per device.

```python
import jax
import jax.numpy as jnp
from jax import lax

V = 1024
O = 240
NR = 4
IROW = 5
PAIR_DEV = 32
LIVE_DEV = 24
I = 160
PAIRS = 4096
N_TILE = 32


def draw_pair_mask(key, part):
    groups = PAIRS // PAIR_DEV
    base = jax.random.fold_in(key, 11)
    key_count, key_full, key_perm = jax.random.split(base, 3)
    counts = jax.random.randint(key_count, (groups,), 1, LIVE_DEV + 1)
    full_group = jax.random.randint(key_full, (), 0, groups)
    sparse_group = (full_group + 1) % groups
    counts = jnp.where(jnp.arange(groups) == full_group, LIVE_DEV, counts)
    counts = jnp.where(jnp.arange(groups) == sparse_group, 1, counts)
    order_ranks = jax.vmap(lambda subkey: jax.random.permutation(subkey, PAIR_DEV))(jax.random.split(key_perm, groups))
    return (order_ranks < counts[:, None]).astype(jnp.int32).reshape(PAIRS)


def with_spikes(result, rng, source, target, blocks, factor):
    owner, partner = [(jnp.arange(result.shape[axis_at]) // (result.shape[axis_at] // blocks)).reshape([-1 if axis == axis_at else 1 for axis in range(result.ndim)]) for axis_at in (source, target)]
    chosen = jax.random.permutation(rng, blocks)[partner]
    strong = (owner == chosen) | (owner == (partner + blocks // 2) % blocks)
    return jnp.where(strong, factor * result, result)


def block_levels(key, dims, shards, low, top_value):
    loudness = 1.0
    for axis_at, parts in shards:
        draws = jax.random.uniform(jax.random.fold_in(jax.random.fold_in(key, 6), axis_at), (parts,), jnp.float32, low / len(shards), top_value / len(shards))
        loudness = loudness * jnp.repeat(jnp.exp(draws), dims[axis_at] // parts).reshape((-1,) + (1,) * (len(dims) - 1 - axis_at))
    return loudness


def centred(own_key, dims, deviation, bound, shards=(), held_as=jnp.bfloat16):
    loudness = block_levels(own_key, dims, shards, -0.22, 0.18) if shards else 1.0
    drawn = jax.random.normal(own_key, dims, jnp.float32) * deviation * loudness
    return jnp.minimum(jnp.maximum(drawn, -bound), bound).astype(held_as)


def noise_with(key, extent, spread, bound, pieces, heavy, held_as=jnp.bfloat16):
    array = spread * jax.random.normal(key, extent, jnp.float32)
    if pieces:
        array = array * block_levels(key, extent, pieces, -0.22, 0.18)
    return jnp.clip(with_spikes(array, jax.random.fold_in(key, 3), *heavy), -bound, bound).astype(held_as)


def setup_inputs(seed: int = 0) -> dict:
    splits = jax.random.split(jax.random.key(seed), 5)
    return {
        "amplitudes": centred(splits[0], (I, NR, PAIRS * O), 1.0, 6.0, ((2, 128),)),
        "w_vvvo": noise_with(splits[1], (V, PAIRS * O), (PAIRS * O) ** -0.5, 0.0234375, ((1, 128),), (1, 0, 128, 5.5)),
        "pair_mask": draw_pair_mask(jax.random.fold_in(splits[4], 71), 0),
        "owner_map": jax.random.permutation(splits[3], N_TILE).astype(jnp.int32),
    }


def reference(amplitudes, w_vvvo, pair_mask, owner_map):
    block_cols = PAIR_DEV * O
    block_total = PAIRS // PAIR_DEV

    def add_block(running, index):
        offset = (index * block_cols).astype(jnp.int32)
        amp_block = lax.dynamic_slice_in_dim(amplitudes, offset, block_cols, 2).astype(jnp.float32)
        mask_part = lax.dynamic_slice_in_dim(pair_mask, (index * PAIR_DEV).astype(jnp.int32), PAIR_DEV, 0)
        mask_cols = jnp.repeat(mask_part.astype(jnp.float32), O)
        w_block = lax.dynamic_slice_in_dim(w_vvvo, offset, block_cols, 1).astype(jnp.float32)
        masked = amp_block * mask_cols
        return running + jnp.einsum("irk,ak->ira", masked, w_block, precision=lax.Precision.HIGHEST), None

    start_value = jnp.zeros((I, NR, V), jnp.float32)
    full_sigma, _ = lax.scan(add_block, start_value, jnp.arange(block_total, dtype=jnp.int32))
    blocked = full_sigma.reshape(N_TILE, IROW, NR, V)
    ordered = jnp.take(blocked, owner_map.astype(jnp.int32), axis=0)
    return ordered.reshape(I, NR, V)
```

```python
import functools

import jax
import jax.numpy as jnp
from jax import lax
from jax.experimental import pallas as pl
from jax.experimental.pallas import tpu as pltpu
from jax.sharding import PartitionSpec as P

AXES = ("grp", "tile")
TORUS = 4
ROWS = 20
UNIT = 2 * ROWS
HALF = 512
VIRT = 256
NT = (((1,), (1,)), ((), ()))
BOUNDS = (0, 512, 1280, 2560, 4608, 7680)
DEPTH = 3


def coords(i):
    g, t = divmod(i, 32)
    z_lo, core = divmod(g, 2)
    x, r = divmod(t, 8)
    z_hi, y = divmod(r, 4)
    return x, y, z_hi * 2 + z_lo, core


def index(x, y, z, core):
    return ((z % 2) * 2 + core) * 32 + x * 8 + (z // 2) * 4 + y


def pairs(move):
    return [(i, index(*move(*coords(i)))) for i in range(128)]


OTHER_CORE = pairs(lambda x, y, z, c: (x, y, z, 1 - c))


def along_own(k):
    return pairs(lambda x, y, z, c: (x, y ^ k, z, c) if c else (x ^ k, y, z, c))


def plane_groups():
    groups = {}
    for i in range(128):
        x, y, z, c = coords(i)
        key, place = ((c, y), (x, z)) if c else ((c, x), (y, z))
        groups.setdefault(key, []).append((place, i))
    return [[i for _, i in sorted(g)] for g in groups.values()]


def mask_row(mask_ref, c0, width, occ):
    col = lax.broadcasted_iota(jnp.int32, (1, width), 1) + c0
    row = jnp.zeros((1, width), jnp.float32)
    for p in range(c0 // occ, (c0 + width - 1) // occ + 1):
        inside = (col >= p * occ) & (col < (p + 1) * occ)
        row = jnp.where(inside, mask_ref[p].astype(jnp.float32), row)
    return row.astype(jnp.bfloat16)


def here():
    g, t = lax.axis_index("grp"), lax.axis_index("tile")
    return lax.rem(g, 2), t // 8, lax.rem(t, 4)


def put(out_ref, total, side, x_here, y_here):
    for x in range(TORUS):
        for y in range(TORUS):
            u = x * TORUS + y
            slot = jnp.where(side == 0, (x ^ x_here) * TORUS + y, (y ^ y_here) * TORUS + x)
            out_ref[slot] = total[u * UNIT : (u + 1) * UNIT]


def columns(k):
    return pl.ds(BOUNDS[k], BOUNDS[k + 1] - BOUNDS[k])


def start_weights(w_ref, w_s, w_sem, side, k):
    for z_lo in range(2):
        pltpu.make_async_copy(
            w_ref.at[z_lo, side, :, columns(k)],
            w_s.at[pl.ds(z_lo * VIRT, VIRT), columns(k)],
            w_sem.at[k],
        ).start()


def wait_for(ref, sem):
    pltpu.make_async_copy(ref, ref, sem).wait()


def first_half(
    occ, owner_hbm, mask_hbm, amp_ref, w_ref, out_ref, x_ref,
    owner_ref, mask_ref, a_s, w_s, acc, a_sem, w_sem, s_sem,
):
    core, x_here, y_here = here()
    side = 1 - core
    blocks = len(BOUNDS) - 1
    rows = a_s.shape[0] // 32
    tables = [
        pltpu.make_async_copy(owner_hbm, owner_ref, s_sem.at[0]),
        pltpu.make_async_copy(mask_hbm, mask_ref, s_sem.at[1]),
    ]
    for table in tables:
        table.start()

    def start_amplitudes(k):
        for x in range(TORUS):
            for y in range(TORUS):
                for z_hi in range(2):
                    source = owner_ref[x * 8 + z_hi * 4 + y]
                    place = (x * TORUS + y) * 2 + z_hi
                    pltpu.make_async_copy(
                        amp_ref.at[pl.ds(source * rows, rows), :, columns(k)],
                        a_s.at[pl.ds(place * rows, rows), :, columns(k)],
                        a_sem.at[k],
                    ).start()

    for k in range(DEPTH):
        start_weights(w_ref, w_s, w_sem, side, k)
    for table in tables:
        table.wait()
    for k in range(DEPTH):
        start_amplitudes(k)
    for k in range(blocks):
        if k + DEPTH < blocks:
            start_weights(w_ref, w_s, w_sem, side, k + DEPTH)
            start_amplitudes(k + DEPTH)
        c0, c1 = BOUNDS[k], BOUNDS[k + 1]
        wait_for(a_s.at[:, :, columns(k)], a_sem.at[k])
        amp = a_s[:, :, c0:c1].reshape(x_ref.shape[0], c1 - c0)
        x_ref[:, c0:c1] = amp * mask_row(mask_ref, c0, c1 - c0, occ)
        wait_for(w_s.at[:, columns(k)], w_sem.at[k])
        part = lax.dot_general(x_ref[:, c0:c1], w_s[:, c0:c1], NT, preferred_element_type=jnp.float32)
        if k == 0:
            acc[...] = part
        elif k < blocks - 1:
            acc[...] += part
        else:
            put(out_ref, acc[...] + part, side, x_here, y_here)


def second_half(x_ref, w_ref, out_ref, w_s, acc, w_sem):
    side, x_here, y_here = here()
    blocks = len(BOUNDS) - 1
    for k in range(DEPTH):
        start_weights(w_ref, w_s, w_sem, side, k)
    for k in range(blocks):
        if k + DEPTH < blocks:
            start_weights(w_ref, w_s, w_sem, side, k + DEPTH)
        c0, c1 = BOUNDS[k], BOUNDS[k + 1]
        wait_for(w_s.at[:, columns(k)], w_sem.at[k])
        part = lax.dot_general(x_ref[:, c0:c1], w_s[:, c0:c1], NT, preferred_element_type=jnp.float32)
        if k == 0:
            acc[...] = part
        elif k < blocks - 1:
            acc[...] += part
        else:
            put(out_ref, acc[...] + part, side, x_here, y_here)


def shards(amplitudes, w_vvvo, pair_mask, owner_map):
    occ_total, roots, cols = amplitudes.shape
    rows = occ_total * roots
    w4 = w_vvvo.reshape(2, 2, VIRT, cols)
    any_spec = pl.BlockSpec(memory_space=pl.ANY)
    hbm = pl.BlockSpec(memory_space=pltpu.HBM)
    vmem = pl.BlockSpec(memory_space=pltpu.VMEM)
    part_shape = pltpu.VMEM((TORUS * TORUS, UNIT, HALF), jnp.float32)
    blocks = len(BOUNDS) - 1
    params = pltpu.CompilerParams(vmem_limit_bytes=40 * 2**20)
    flops = 2 * rows * HALF * cols
    theirs, masked = pl.pallas_call(
        functools.partial(first_half, cols // pair_mask.shape[0]),
        in_specs=[any_spec, any_spec, hbm, hbm],
        out_specs=[vmem, vmem],
        out_shape=[part_shape, pltpu.VMEM((rows, cols), jnp.bfloat16)],
        scratch_shapes=[
            pltpu.SMEM(owner_map.shape, jnp.int32),
            pltpu.SMEM(pair_mask.shape, jnp.int32),
            pltpu.VMEM(amplitudes.shape, jnp.bfloat16),
            pltpu.VMEM((HALF, cols), jnp.bfloat16),
            pltpu.VMEM((rows, HALF), jnp.float32),
            pltpu.SemaphoreType.DMA((blocks,)),
            pltpu.SemaphoreType.DMA((blocks,)),
            pltpu.SemaphoreType.DMA((2,)),
        ],
        compiler_params=params,
        cost_estimate=pl.CostEstimate(flops=flops, bytes_accessed=18 * 10**6, transcendentals=0),
        name="their_half",
    )(owner_map, pair_mask, amplitudes, w4)
    from_core = lax.ppermute(theirs, AXES, OTHER_CORE)
    own = pl.pallas_call(
        second_half,
        in_specs=[vmem, hbm],
        out_specs=vmem,
        out_shape=part_shape,
        scratch_shapes=[
            pltpu.VMEM((HALF, cols), jnp.bfloat16),
            pltpu.VMEM((rows, HALF), jnp.float32),
            pltpu.SemaphoreType.DMA((blocks,)),
        ],
        compiler_params=params,
        cost_estimate=pl.CostEstimate(flops=flops, bytes_accessed=8 * 10**6, transcendentals=0),
        name="own_half",
    )(masked, w4)
    chip = (own + from_core).reshape(TORUS, TORUS, UNIT, HALF)
    arrived = [lax.ppermute(chip[k], AXES, along_own(k)) for k in (2, 1, 3)]
    plane = chip[0] + arrived[0] + arrived[1] + arrived[2]
    sent = plane.reshape(TORUS, 2, ROWS, 2, VIRT).transpose(0, 1, 3, 2, 4).reshape(16, ROWS, VIRT)
    got = lax.all_to_all(sent, AXES, 0, 0, axis_index_groups=plane_groups(), tiled=True)
    return got.sum(axis=0).reshape(ROWS // roots, roots, VIRT)


def solution(mesh):
    return jax.shard_map(
        shards,
        mesh=mesh,
        in_specs=(P(None, None, AXES), P(None, AXES), P(AXES), P()),
        out_specs=P("tile", None, "grp"),
        check_vma=False,
    )
```

```python
import functools

import jax
import jax.numpy as jnp
from jax import lax
from jax.experimental import pallas as pl
from jax.experimental.pallas import tpu as pltpu
from jax.sharding import PartitionSpec as P

AXES = ("grp", "tile")
TORUS = 4
ROWS = 20
UNIT = 2 * ROWS
HALF = 512
VIRT = 256
NT = (((1,), (1,)), ((), ()))
ORDER = (2, 1, 3, 0)
SPLIT = (0, 3, 4)
FIRST = (0, 768, 2304, 4096, 5888, 7168, 7680)
OWN = (0, 7680)
DEPTH = 2


def coords(i):
    g, t = divmod(i, 32)
    z_lo, core = divmod(g, 2)
    x, r = divmod(t, 8)
    z_hi, y = divmod(r, 4)
    return x, y, z_hi * 2 + z_lo, core


def index(x, y, z, core):
    return ((z % 2) * 2 + core) * 32 + x * 8 + (z // 2) * 4 + y


def pairs(move):
    return [(i, index(*move(*coords(i)))) for i in range(128)]


OTHER_CORE = pairs(lambda x, y, z, c: (x, y, z, 1 - c))


def along_own(k):
    return pairs(lambda x, y, z, c: (x, y ^ k, z, c) if c else (x ^ k, y, z, c))


def plane_groups():
    groups = {}
    for i in range(128):
        x, y, z, c = coords(i)
        key, place = ((c, y), (x, z)) if c else ((c, x), (y, z))
        groups.setdefault(key, []).append((place, i))
    return [[i for _, i in sorted(g)] for g in groups.values()]


def mask_row(mask_ref, c0, width, occ):
    col = lax.broadcasted_iota(jnp.int32, (1, width), 1) + c0
    row = jnp.zeros((1, width), jnp.float32)
    for p in range(c0 // occ, (c0 + width - 1) // occ + 1):
        inside = (col >= p * occ) & (col < (p + 1) * occ)
        row = jnp.where(inside, mask_ref[p].astype(jnp.float32), row)
    return row.astype(jnp.bfloat16)


def here():
    g, t = lax.axis_index("grp"), lax.axis_index("tile")
    core, x, y = lax.rem(g, 2), t // 8, lax.rem(t, 4)
    return core, jnp.where(core == 0, x, y), jnp.where(core == 0, y, x)


def columns(bounds, k):
    return pl.ds(bounds[k], bounds[k + 1] - bounds[k])


def start_weights(w_ref, w_s, sem, side, cols):
    for z_lo in range(2):
        pltpu.make_async_copy(
            w_ref.at[z_lo, side, :, cols], w_s.at[pl.ds(z_lo * VIRT, VIRT), cols], sem
        ).start()


def wait_for(ref, sem):
    pltpu.make_async_copy(ref, ref, sem).wait()


def first_half(
    occ, owner_hbm, mask_hbm, amp_ref, w_ref, out_ref, x_ref, w_own,
    owner_ref, mask_ref, a_s, w_s, acc, a_sem, w_sem, own_sem, s_sem,
):
    core, own_at, other_at = here()
    blocks = len(FIRST) - 1
    rows = a_s.shape[0] // 32
    tables = [
        pltpu.make_async_copy(owner_hbm, owner_ref, s_sem.at[0]),
        pltpu.make_async_copy(mask_hbm, mask_ref, s_sem.at[1]),
    ]
    for table in tables:
        table.start()
    own_step, other_step = jnp.where(core == 0, 8, 1), jnp.where(core == 0, 1, 8)

    def start_amplitudes(k):
        for p, shift in enumerate(ORDER):
            for j in range(TORUS):
                for z_hi in range(2):
                    source = owner_ref[(own_at ^ shift) * own_step + j * other_step + z_hi * 4]
                    place = (p * TORUS + j) * 2 + z_hi
                    pltpu.make_async_copy(
                        amp_ref.at[pl.ds(source * rows, rows), :, columns(FIRST, k)],
                        a_s.at[pl.ds(place * rows, rows), :, columns(FIRST, k)],
                        a_sem.at[k],
                    ).start()

    for k in range(DEPTH):
        start_weights(w_ref, w_s, w_sem.at[k], 1 - core, columns(FIRST, k))
    for table in tables:
        table.wait()
    for k in range(DEPTH):
        start_amplitudes(k)
    for k in range(blocks):
        if k + DEPTH < blocks:
            start_weights(w_ref, w_s, w_sem.at[k + DEPTH], 1 - core, columns(FIRST, k + DEPTH))
            start_amplitudes(k + DEPTH)
        elif k < blocks - 1:
            n = k + DEPTH - blocks
            start_weights(w_ref, w_own, own_sem.at[n], core, columns(OWN, n))
        c0, c1 = FIRST[k], FIRST[k + 1]
        wait_for(a_s.at[:, :, columns(FIRST, k)], a_sem.at[k])
        amp = a_s[:, :, c0:c1].reshape(x_ref.shape[0], c1 - c0)
        x_ref[:, c0:c1] = amp * mask_row(mask_ref, c0, c1 - c0, occ)
        wait_for(w_s.at[:, columns(FIRST, k)], w_sem.at[k])
        part = lax.dot_general(x_ref[:, c0:c1], w_s[:, c0:c1], NT, preferred_element_type=jnp.float32)
        if k == 0:
            acc[...] = part
        elif k < blocks - 1:
            acc[...] += part
        else:
            total = acc[...] + part
            for p, shift in enumerate(ORDER):
                for j in range(TORUS):
                    u = p * TORUS + j
                    hop = j ^ other_at
                    at = jnp.where(hop == 0, 3, jnp.where(hop == 3, 2, jnp.where(hop == 2, 0, 1)))
                    out_ref[at, own_at ^ shift] = total[u * UNIT : (u + 1) * UNIT]
    for n in range(len(OWN) - 1):
        wait_for(w_own.at[:, columns(OWN, n)], own_sem.at[n])


def own_part(r0, r1, x_ref, w_ref, out_ref):
    part = lax.dot_general(x_ref[r0:r1], w_ref[...], NT, preferred_element_type=jnp.float32)
    out_ref[...] = part.reshape(out_ref.shape)


def shards(amplitudes, w_vvvo, pair_mask, owner_map):
    occ_total, roots, cols = amplitudes.shape
    rows = occ_total * roots
    w4 = w_vvvo.reshape(2, 2, VIRT, cols)
    any_spec = pl.BlockSpec(memory_space=pl.ANY)
    hbm = pl.BlockSpec(memory_space=pltpu.HBM)
    vmem = pl.BlockSpec(memory_space=pltpu.VMEM)

    def params(kib):
        return pltpu.CompilerParams(vmem_limit_bytes=kib * 1024)

    def cost(some_rows, moved):
        return pl.CostEstimate(flops=2 * some_rows * HALF * cols, bytes_accessed=moved, transcendentals=0)

    def part_shape(chunks):
        return pltpu.VMEM((chunks, TORUS, UNIT, HALF), jnp.float32)

    theirs, masked, weights = pl.pallas_call(
        functools.partial(first_half, cols // pair_mask.shape[0]),
        in_specs=[any_spec, any_spec, hbm, hbm],
        out_specs=[vmem, vmem, vmem],
        out_shape=[
            part_shape(TORUS),
            pltpu.VMEM((rows, cols), jnp.bfloat16),
            pltpu.VMEM((HALF, cols), jnp.bfloat16),
        ],
        scratch_shapes=[
            pltpu.SMEM(owner_map.shape, jnp.int32),
            pltpu.SMEM(pair_mask.shape, jnp.int32),
            pltpu.VMEM(amplitudes.shape, jnp.bfloat16),
            pltpu.VMEM((HALF, cols), jnp.bfloat16),
            pltpu.VMEM((rows, HALF), jnp.float32),
            pltpu.SemaphoreType.DMA((len(FIRST) - 1,)),
            pltpu.SemaphoreType.DMA((len(FIRST) - 1,)),
            pltpu.SemaphoreType.DMA((len(OWN) - 1,)),
            pltpu.SemaphoreType.DMA((2,)),
        ],
        compiler_params=params(43000),
        cost_estimate=cost(rows, 26 * 10**6),
        name="their_half",
    )(owner_map, pair_mask, amplitudes, w4)
    from_core = lax.ppermute(theirs, AXES, OTHER_CORE)
    chunk = rows // TORUS
    parts = []
    for n, (a, b) in enumerate(zip(SPLIT[:-1], SPLIT[1:])):
        parts.append(
            pl.pallas_call(
                functools.partial(own_part, a * chunk, b * chunk),
                in_specs=[vmem, vmem],
                out_specs=vmem,
                out_shape=part_shape(b - a),
                compiler_params=params(16000),
                cost_estimate=cost((b - a) * chunk, 0),
                name=f"own_part_{n}",
            )(masked, weights)
        )
    total = []
    for n, (a, b) in enumerate(zip(SPLIT[:-1], SPLIT[1:])):
        total += [parts[n][i - a] + from_core[i] for i in range(a, b)]
    arrived = [lax.ppermute(total[p], AXES, along_own(shift)) for p, shift in enumerate(ORDER) if shift]
    plane = total[-1] + arrived[0] + arrived[1] + arrived[2]
    sent = plane.reshape(TORUS, 2, ROWS, 2, VIRT).transpose(0, 1, 3, 2, 4).reshape(16, ROWS, VIRT)
    got = lax.all_to_all(sent, AXES, 0, 0, axis_index_groups=plane_groups(), tiled=True)
    return got.sum(axis=0).reshape(ROWS // roots, roots, VIRT)


def solution(mesh):
    return jax.shard_map(
        shards,
        mesh=mesh,
        in_specs=(P(None, None, AXES), P(None, AXES), P(AXES), P()),
        out_specs=P("tile", None, "grp"),
        check_vma=False,
    )
```

```python
import functools

import jax
import jax.numpy as jnp
from jax import lax
from jax.experimental import pallas as pl
from jax.experimental.pallas import tpu as pltpu
from jax.sharding import PartitionSpec as P

AXES = ("grp", "tile")
TORUS = 4
ROWS = 20
UNIT = 2 * ROWS
HALF = 512
VIRT = 256
NT = (((1,), (1,)), ((), ()))
ORDER = (3, 1, 2, 0)
FIRST = (0, 768, 2304, 4096, 5888, 7168, 7680)
OWN = (0, 7680)
DEPTH = 2


def coords(i):
    g, t = divmod(i, 32)
    z_lo, core = divmod(g, 2)
    x, r = divmod(t, 8)
    z_hi, y = divmod(r, 4)
    return x, y, z_hi * 2 + z_lo, core


def index(x, y, z, core):
    return ((z % 2) * 2 + core) * 32 + x * 8 + (z // 2) * 4 + y


def pairs(move):
    return [(i, index(*move(*coords(i)))) for i in range(128)]


OTHER_CORE = pairs(lambda x, y, z, c: (x, y, z, 1 - c))


def along_own(k):
    return pairs(lambda x, y, z, c: (x, y ^ k, z, c) if c else (x ^ k, y, z, c))


def plane_groups():
    groups = {}
    for i in range(128):
        x, y, z, c = coords(i)
        key, place = ((c, y), (x, z)) if c else ((c, x), (y, z))
        groups.setdefault(key, []).append((place, i))
    return [[i for _, i in sorted(g)] for g in groups.values()]


def mask_row(mask_ref, c0, width, occ):
    col = lax.broadcasted_iota(jnp.int32, (1, width), 1) + c0
    row = jnp.zeros((1, width), jnp.float32)
    for p in range(c0 // occ, (c0 + width - 1) // occ + 1):
        inside = (col >= p * occ) & (col < (p + 1) * occ)
        row = jnp.where(inside, mask_ref[p].astype(jnp.float32), row)
    return row.astype(jnp.bfloat16)


def here():
    g, t = lax.axis_index("grp"), lax.axis_index("tile")
    core, x, y = lax.rem(g, 2), t // 8, lax.rem(t, 4)
    return core, jnp.where(core == 0, x, y), jnp.where(core == 0, y, x)


def columns(bounds, k):
    return pl.ds(bounds[k], bounds[k + 1] - bounds[k])


def start_weights(w_ref, w_s, sem, side, cols):
    for z_lo in range(2):
        pltpu.make_async_copy(
            w_ref.at[z_lo, side, :, cols], w_s.at[pl.ds(z_lo * VIRT, VIRT), cols], sem
        ).start()


def wait_for(ref, sem):
    pltpu.make_async_copy(ref, ref, sem).wait()


def first_half(
    occ, owner_hbm, mask_hbm, amp_ref, w_ref, out_ref, x_ref, w_own,
    owner_ref, mask_ref, a_s, w_s, acc, a_sem, w_sem, own_sem, s_sem,
):
    core, own_at, other_at = here()
    blocks = len(FIRST) - 1
    rows = a_s.shape[0] // 32
    tables = [
        pltpu.make_async_copy(owner_hbm, owner_ref, s_sem.at[0]),
        pltpu.make_async_copy(mask_hbm, mask_ref, s_sem.at[1]),
    ]
    for table in tables:
        table.start()
    own_step, other_step = jnp.where(core == 0, 8, 1), jnp.where(core == 0, 1, 8)

    def start_amplitudes(k):
        for p, shift in enumerate(ORDER):
            for j in range(TORUS):
                for z_hi in range(2):
                    source = owner_ref[(own_at ^ shift) * own_step + j * other_step + z_hi * 4]
                    place = (p * TORUS + j) * 2 + z_hi
                    pltpu.make_async_copy(
                        amp_ref.at[pl.ds(source * rows, rows), :, columns(FIRST, k)],
                        a_s.at[pl.ds(place * rows, rows), :, columns(FIRST, k)],
                        a_sem.at[k],
                    ).start()

    for k in range(DEPTH):
        start_weights(w_ref, w_s, w_sem.at[k], 1 - core, columns(FIRST, k))
    for table in tables:
        table.wait()
    for k in range(DEPTH):
        start_amplitudes(k)
    for k in range(blocks):
        if k + DEPTH < blocks:
            start_weights(w_ref, w_s, w_sem.at[k + DEPTH], 1 - core, columns(FIRST, k + DEPTH))
            start_amplitudes(k + DEPTH)
        elif k < blocks - 1:
            n = k + DEPTH - blocks
            start_weights(w_ref, w_own, own_sem.at[n], core, columns(OWN, n))
        c0, c1 = FIRST[k], FIRST[k + 1]
        wait_for(a_s.at[:, :, columns(FIRST, k)], a_sem.at[k])
        amp = a_s[:, :, c0:c1].reshape(x_ref.shape[0], c1 - c0)
        x_ref[:, c0:c1] = amp * mask_row(mask_ref, c0, c1 - c0, occ)
        wait_for(w_s.at[:, columns(FIRST, k)], w_sem.at[k])
        part = lax.dot_general(x_ref[:, c0:c1], w_s[:, c0:c1], NT, preferred_element_type=jnp.float32)
        if k == 0:
            acc[...] = part
        elif k < blocks - 1:
            acc[...] += part
        else:
            total = acc[...] + part
            for p, shift in enumerate(ORDER):
                for j in range(TORUS):
                    u = p * TORUS + j
                    hop = j ^ other_at
                    at = sum(jnp.where(hop == h, n, 0) for n, h in enumerate(ORDER))
                    out_ref[at, own_at ^ shift] = total[u * UNIT : (u + 1) * UNIT]
    for n in range(len(OWN) - 1):
        wait_for(w_own.at[:, columns(OWN, n)], own_sem.at[n])


def product(x_ref, r0, r1, c0, w_ref):
    return lax.dot_general(
        x_ref[r0:r1, c0 : c0 + w_ref.shape[1]], w_ref[...], NT, preferred_element_type=jnp.float32
    )


def own_part(r0, r1, x_ref, w_ref, out_ref):
    out_ref[...] = product(x_ref, r0, r1, 0, w_ref).reshape(out_ref.shape)


def plane_sum(kept_ref, core_ref, a_ref, b_ref, c_ref, out_ref):
    for j in range(TORUS):
        for z_hi in range(2):
            rows = slice(z_hi * ROWS, (z_hi + 1) * ROWS)
            total = kept_ref[0, j, rows] + core_ref[TORUS - 1, j, rows]
            total = ((total + a_ref[j, rows]) + b_ref[j, rows]) + c_ref[j, rows]
            for z_lo in range(2):
                n = (j * 2 + z_hi) * 2 + z_lo
                out_ref[n] = total[:, z_lo * VIRT : (z_lo + 1) * VIRT].reshape(out_ref.shape[1:])


def shards(amplitudes, w_vvvo, pair_mask, owner_map):
    occ_total, roots, cols = amplitudes.shape
    rows = occ_total * roots
    w4 = w_vvvo.reshape(2, 2, VIRT, cols)
    any_spec = pl.BlockSpec(memory_space=pl.ANY)
    hbm = pl.BlockSpec(memory_space=pltpu.HBM)
    vmem = pl.BlockSpec(memory_space=pltpu.VMEM)

    def params(kib):
        return pltpu.CompilerParams(vmem_limit_bytes=kib * 1024)

    def cost(some_rows, moved):
        return pl.CostEstimate(flops=2 * some_rows * HALF * cols, bytes_accessed=moved, transcendentals=0)

    def part_shape(chunks):
        return pltpu.VMEM((chunks, TORUS, UNIT, HALF), jnp.float32)

    theirs, masked, weights = pl.pallas_call(
        functools.partial(first_half, cols // pair_mask.shape[0]),
        in_specs=[any_spec, any_spec, hbm, hbm],
        out_specs=[vmem, vmem, vmem],
        out_shape=[
            part_shape(TORUS),
            pltpu.VMEM((rows, cols), jnp.bfloat16),
            pltpu.VMEM((HALF, OWN[-1]), jnp.bfloat16),
        ],
        scratch_shapes=[
            pltpu.SMEM(owner_map.shape, jnp.int32),
            pltpu.SMEM(pair_mask.shape, jnp.int32),
            pltpu.VMEM(amplitudes.shape, jnp.bfloat16),
            pltpu.VMEM((HALF, cols), jnp.bfloat16),
            pltpu.VMEM((rows, HALF), jnp.float32),
            pltpu.SemaphoreType.DMA((len(FIRST) - 1,)),
            pltpu.SemaphoreType.DMA((len(FIRST) - 1,)),
            pltpu.SemaphoreType.DMA((len(OWN) - 1,)),
            pltpu.SemaphoreType.DMA((2,)),
        ],
        compiler_params=params(43000),
        cost_estimate=cost(rows, 26 * 10**6),
        name="their_half",
    )(owner_map, pair_mask, amplitudes, w4)
    from_core = lax.ppermute(theirs, AXES, OTHER_CORE)
    chunk = rows // TORUS
    sent_rows = (TORUS - 1) * chunk

    def own(r0, r1, name):
        return pl.pallas_call(
            functools.partial(own_part, r0, r1),
            in_specs=[vmem, vmem],
            out_specs=vmem,
            out_shape=part_shape((r1 - r0) // chunk),
            compiler_params=params(16000),
            cost_estimate=cost(r1 - r0, 0),
            name=name,
        )(masked, weights)

    leaving = own(0, sent_rows, "own_sent")
    kept = own(sent_rows, rows, "own_kept")
    arrived = [
        lax.ppermute(leaving[p] + from_core[p], AXES, along_own(shift))
        for p, shift in enumerate(ORDER)
        if shift
    ]
    sent = pl.pallas_call(
        plane_sum,
        in_specs=[vmem] * 5,
        out_specs=vmem,
        out_shape=pltpu.VMEM((16, ROWS // roots, roots, VIRT), jnp.float32),
        compiler_params=params(16000),
        name="plane_sum",
    )(kept, from_core, *arrived)
    got = lax.all_to_all(sent, AXES, 0, 0, axis_index_groups=plane_groups(), tiled=True)
    return got.sum(axis=0)


def solution(mesh):
    return jax.shard_map(
        shards,
        mesh=mesh,
        in_specs=(P(None, None, AXES), P(None, AXES), P(AXES), P()),
        out_specs=P("tile", None, "grp"),
        check_vma=False,
    )
```

```python
import functools

import jax
import jax.numpy as jnp
from jax import lax
from jax.experimental import pallas as pl
from jax.experimental.pallas import tpu as pltpu
from jax.sharding import PartitionSpec as P

AXES = ("grp", "tile")
TORUS = 4
ROWS = 20
UNIT = 2 * ROWS
HALF = 512
VIRT = 256
NT = (((1,), (1,)), ((), ()))
ORDER = (3, 1, 2, 0)
FIRST = (0, 768, 2304, 4096, 5888, 7168, 7680)
OWN = (0, 2560, 5120, 7680)
DEPTH = 2


def coords(i):
    g, t = divmod(i, 32)
    z_lo, core = divmod(g, 2)
    x, r = divmod(t, 8)
    z_hi, y = divmod(r, 4)
    return x, y, z_hi * 2 + z_lo, core


def index(x, y, z, core):
    return ((z % 2) * 2 + core) * 32 + x * 8 + (z // 2) * 4 + y


def pairs(move):
    return [(i, index(*move(*coords(i)))) for i in range(128)]


OTHER_CORE = pairs(lambda x, y, z, c: (x, y, z, 1 - c))


def along_own(k):
    return pairs(lambda x, y, z, c: (x, y ^ k, z, c) if c else (x ^ k, y, z, c))


def plane_groups():
    groups = {}
    for i in range(128):
        x, y, z, c = coords(i)
        key, place = ((c, y), (x, z)) if c else ((c, x), (y, z))
        groups.setdefault(key, []).append((place, i))
    return [[i for _, i in sorted(g)] for g in groups.values()]


def mask_row(mask_ref, c0, width, occ):
    col = lax.broadcasted_iota(jnp.int32, (1, width), 1) + c0
    row = jnp.zeros((1, width), jnp.float32)
    for p in range(c0 // occ, (c0 + width - 1) // occ + 1):
        inside = (col >= p * occ) & (col < (p + 1) * occ)
        row = jnp.where(inside, mask_ref[p].astype(jnp.float32), row)
    return row.astype(jnp.bfloat16)


def here():
    g, t = lax.axis_index("grp"), lax.axis_index("tile")
    core, x, y = lax.rem(g, 2), t // 8, lax.rem(t, 4)
    return core, jnp.where(core == 0, x, y), jnp.where(core == 0, y, x)


def columns(bounds, k):
    return pl.ds(bounds[k], bounds[k + 1] - bounds[k])


def start_weights(w_ref, w_s, sem, side, cols):
    for z_lo in range(2):
        pltpu.make_async_copy(
            w_ref.at[z_lo, side, :, cols], w_s.at[pl.ds(z_lo * VIRT, VIRT), cols], sem
        ).start()


def wait_for(ref, sem):
    pltpu.make_async_copy(ref, ref, sem).wait()


def first_half(
    occ, owner_hbm, mask_hbm, amp_ref, w_ref, out_ref, x_ref, w_own,
    owner_ref, mask_ref, a_s, w_s, acc, a_sem, w_sem, own_sem, s_sem,
):
    core, own_at, other_at = here()
    blocks = len(FIRST) - 1
    rows = a_s.shape[0] // 32
    tables = [
        pltpu.make_async_copy(owner_hbm, owner_ref, s_sem.at[0]),
        pltpu.make_async_copy(mask_hbm, mask_ref, s_sem.at[1]),
    ]
    for table in tables:
        table.start()
    own_step, other_step = jnp.where(core == 0, 8, 1), jnp.where(core == 0, 1, 8)

    def start_amplitudes(k):
        for p, shift in enumerate(ORDER):
            for j in range(TORUS):
                for z_hi in range(2):
                    source = owner_ref[(own_at ^ shift) * own_step + j * other_step + z_hi * 4]
                    place = (p * TORUS + j) * 2 + z_hi
                    pltpu.make_async_copy(
                        amp_ref.at[pl.ds(source * rows, rows), :, columns(FIRST, k)],
                        a_s.at[pl.ds(place * rows, rows), :, columns(FIRST, k)],
                        a_sem.at[k],
                    ).start()

    for k in range(DEPTH):
        start_weights(w_ref, w_s, w_sem.at[k], 1 - core, columns(FIRST, k))
    for table in tables:
        table.wait()
    for k in range(DEPTH):
        start_amplitudes(k)
    for k in range(blocks):
        if k + DEPTH < blocks:
            start_weights(w_ref, w_s, w_sem.at[k + DEPTH], 1 - core, columns(FIRST, k + DEPTH))
            start_amplitudes(k + DEPTH)
        n = k + len(OWN) - blocks
        if 0 <= n < len(OWN) - 1:
            start_weights(w_ref, w_own, own_sem.at[n], core, columns(OWN, n))
        c0, c1 = FIRST[k], FIRST[k + 1]
        wait_for(a_s.at[:, :, columns(FIRST, k)], a_sem.at[k])
        amp = a_s[:, :, c0:c1].reshape(x_ref.shape[0], c1 - c0)
        x_ref[:, c0:c1] = amp * mask_row(mask_ref, c0, c1 - c0, occ)
        wait_for(w_s.at[:, columns(FIRST, k)], w_sem.at[k])
        part = lax.dot_general(x_ref[:, c0:c1], w_s[:, c0:c1], NT, preferred_element_type=jnp.float32)
        if k == 0:
            acc[...] = part
        elif k < blocks - 1:
            acc[...] += part
        else:
            total = acc[...] + part
            for p, shift in enumerate(ORDER):
                for j in range(TORUS):
                    u = p * TORUS + j
                    hop = j ^ other_at
                    at = sum(jnp.where(hop == h, n, 0) for n, h in enumerate(ORDER))
                    out_ref[at, own_at ^ shift] = total[u * UNIT : (u + 1) * UNIT]
    for n in range(len(OWN) - 1):
        wait_for(w_own.at[:, columns(OWN, n)], own_sem.at[n])


def product(x_ref, r0, r1, c0, w_ref):
    return lax.dot_general(
        x_ref[r0:r1, c0 : c0 + w_ref.shape[1]], w_ref[...], NT, preferred_element_type=jnp.float32
    )


def own_part(r0, r1, x_ref, w_ref, out_ref):
    out_ref[...] = product(x_ref, r0, r1, 0, w_ref).reshape(out_ref.shape)


def plane_sum(kept_ref, core_ref, a_ref, b_ref, c_ref, out_ref):
    for j in range(TORUS):
        for z_hi in range(2):
            rows = slice(z_hi * ROWS, (z_hi + 1) * ROWS)
            total = kept_ref[0, j, rows] + core_ref[TORUS - 1, j, rows]
            total = ((total + a_ref[j, rows]) + b_ref[j, rows]) + c_ref[j, rows]
            for z_lo in range(2):
                n = (j * 2 + z_hi) * 2 + z_lo
                out_ref[n] = total[:, z_lo * VIRT : (z_lo + 1) * VIRT].reshape(out_ref.shape[1:])


def shards(amplitudes, w_vvvo, pair_mask, owner_map):
    occ_total, roots, cols = amplitudes.shape
    rows = occ_total * roots
    w4 = w_vvvo.reshape(2, 2, VIRT, cols)
    any_spec = pl.BlockSpec(memory_space=pl.ANY)
    hbm = pl.BlockSpec(memory_space=pltpu.HBM)
    vmem = pl.BlockSpec(memory_space=pltpu.VMEM)

    def params(kib):
        return pltpu.CompilerParams(vmem_limit_bytes=kib * 1024)

    def cost(some_rows, moved):
        return pl.CostEstimate(flops=2 * some_rows * HALF * cols, bytes_accessed=moved, transcendentals=0)

    def part_shape(chunks):
        return pltpu.VMEM((chunks, TORUS, UNIT, HALF), jnp.float32)

    theirs, masked, weights = pl.pallas_call(
        functools.partial(first_half, cols // pair_mask.shape[0]),
        in_specs=[any_spec, any_spec, hbm, hbm],
        out_specs=[vmem, vmem, vmem],
        out_shape=[
            part_shape(TORUS),
            pltpu.VMEM((rows, cols), jnp.bfloat16),
            pltpu.VMEM((HALF, OWN[-1]), jnp.bfloat16),
        ],
        scratch_shapes=[
            pltpu.SMEM(owner_map.shape, jnp.int32),
            pltpu.SMEM(pair_mask.shape, jnp.int32),
            pltpu.VMEM(amplitudes.shape, jnp.bfloat16),
            pltpu.VMEM((HALF, cols), jnp.bfloat16),
            pltpu.VMEM((rows, HALF), jnp.float32),
            pltpu.SemaphoreType.DMA((len(FIRST) - 1,)),
            pltpu.SemaphoreType.DMA((len(FIRST) - 1,)),
            pltpu.SemaphoreType.DMA((len(OWN) - 1,)),
            pltpu.SemaphoreType.DMA((2,)),
        ],
        compiler_params=params(43000),
        cost_estimate=cost(rows, 26 * 10**6),
        name="their_half",
    )(owner_map, pair_mask, amplitudes, w4)
    from_core = lax.ppermute(theirs, AXES, OTHER_CORE)
    chunk = rows // TORUS
    sent_rows = (TORUS - 1) * chunk

    def own(r0, r1, name):
        return pl.pallas_call(
            functools.partial(own_part, r0, r1),
            in_specs=[vmem, vmem],
            out_specs=vmem,
            out_shape=part_shape((r1 - r0) // chunk),
            compiler_params=params(16000),
            cost_estimate=cost(r1 - r0, 0),
            name=name,
        )(masked, weights)

    leaving = own(0, sent_rows, "own_sent")
    kept = own(sent_rows, rows, "own_kept")
    arrived = [
        lax.ppermute(leaving[p] + from_core[p], AXES, along_own(shift))
        for p, shift in enumerate(ORDER)
        if shift
    ]
    sent = pl.pallas_call(
        plane_sum,
        in_specs=[vmem] * 5,
        out_specs=vmem,
        out_shape=pltpu.VMEM((16, ROWS // roots, roots, VIRT), jnp.float32),
        compiler_params=params(16000),
        name="plane_sum",
    )(kept, from_core, *arrived)
    got = lax.all_to_all(sent, AXES, 0, 0, axis_index_groups=plane_groups(), tiled=True)
    return got.sum(axis=0)


def solution(mesh):
    return jax.shard_map(
        shards,
        mesh=mesh,
        in_specs=(P(None, None, AXES), P(None, AXES), P(AXES), P()),
        out_specs=P("tile", None, "grp"),
        check_vma=False,
    )
```
